256 devices in a mesh: gx: 4 (over x), gy: 4 (over y), gz: 16 (over z, core).
Axes of the slice: x: 4, y: 4, z: 8, core: 2. Of those that a mesh axis runs over, the one named last changes fastest.
Arguments:
- embeds: bfloat16 [2048, 128, 2048], P(('gx', 'gy', 'gz')), may hold values from -6 to 6
- dest_device: int32 [2048], P(('gx', 'gy', 'gz')), may hold values from 0 to 255, as said below
- shuffle_key: int32 [2048], P(('gx', 'gy', 'gz')), may hold values from 0 to 2047, each once
- lengths: int32 [64], replicated, may hold values from 1 to 4096
- gain: float32 [2048], replicated, may hold values from 0.1 to 1.9
Outputs:
- packed: bfloat16 [4096, 128, 2048], P(('gx', 'gy', 'gz'))
The draws below stay inside these ranges and needn't reach their ends.
Inputs may be any that keep to these rules, and one draw needn't show every extreme that they name: `dest_device`: device numbers are ((gx * 4) + gy) * 16 + gz. A device receives at most 16 tiles, and in every draw some devices receive exactly 16. The 16 devices sharing gx and gy send at most one tile to any one device and exactly 8 tiles to the devices of each gz index. Of one device's tiles at most 1 go to devices of one gz index, and some device reaches that.
All inputs are finite; a program needn't handle non-finite values.
Results may differ from the reference program's by a relative error of at most 0.001.
Values may be sent and summed in bfloat16 or wider, within the bound.
A program may use at most 128 MiB of HBM per device.

```python
import jax
import jax.numpy as jnp
from jax import lax

D = 2048
TILE = 128
TILES_SEQ = 32
TILES_DEV = 8
DEPTH = 16
GROUPS = 16
CAP = 16
TILES = 2048
SEQ_LEN = 4096
SEQS = 64


def draw_dest_device(key, part):
    k_amount, k_label, k_column, k_shift = jax.random.split(key, 4)
    half = GROUPS // 2
    amount = jax.random.randint(k_amount, (DEPTH, half), 0, TILES_DEV + 1)
    amount = amount.at[:, 0].set(TILES_DEV)
    loads = jnp.concatenate([TILES_DEV + amount, TILES_DEV - amount], axis=1)
    labels = jax.vmap(lambda k: jax.random.permutation(k, GROUPS))(jax.random.split(k_label, DEPTH))
    columns = jax.vmap(lambda k: jax.random.permutation(k, GROUPS))(jax.random.split(k_column, DEPTH))
    shift = jax.random.randint(k_shift, (GROUPS,), 0, DEPTH)
    ends = jnp.cumsum(loads, axis=1)
    group = jnp.arange(GROUPS)[:, None, None]
    height = jnp.arange(DEPTH)[None, :, None]
    local = jnp.arange(TILES_DEV)[None, None, :]
    within = height * TILES_DEV + local
    target_z = (within + shift[:, None, None]) % DEPTH
    order = within // DEPTH
    column = columns[target_z, group]
    spot = column + GROUPS * order
    label_index = jnp.sum((spot[..., None] >= ends[target_z]).astype(jnp.int32), axis=-1)
    target_group = labels[target_z, label_index]
    return (target_group * DEPTH + target_z).reshape(-1).astype(jnp.int32)


def set_ends(array, rng, low, largest):
    place = [jax.random.randint(jax.random.fold_in(rng, axis), (), 0, length) for axis, length in enumerate(array.shape)]
    longest = array.shape.index(max(array.shape))
    beside = place[:longest] + [(place[longest] + 1) % array.shape[longest]] + place[longest + 1:]
    return array.at[tuple(place)].set(low).at[tuple(beside)].set(largest)


def steps_of(stream_key, dims, cuts, least, largest):
    level = 1.0
    for dim, shards_of in cuts:
        draws = jax.random.uniform(jax.random.fold_in(jax.random.fold_in(stream_key, 6), dim), (shards_of,), jnp.float32, least / len(cuts), largest / len(cuts))
        level = level * jnp.repeat(jnp.exp(draws), dims[dim] // shards_of).reshape((-1,) + (1,) * (len(dims) - 1 - dim))
    return level


def centred(own_key, dims, scale, most, shards=(), kind=jnp.bfloat16):
    result = jax.random.normal(own_key, dims, jnp.float32) * scale
    if len(shards) > 0:
        result = steps_of(own_key, dims, shards, -0.22, 0.18) * result
    return jnp.clip(result, min=-most, max=most).astype(kind)


def setup_inputs(seed: int = 0) -> dict:
    streams_of = jax.random.split(jax.random.key(seed), 6)
    embeds = centred(streams_of[0], (TILES, TILE, D), 1.0, 6.0, ((0, 256),))
    dest_device = draw_dest_device(jax.random.fold_in(streams_of[5], 71), 0)
    shuffle_key = jax.random.permutation(streams_of[2], TILES).astype(jnp.int32)
    lengths = set_ends(jax.random.randint(streams_of[3], (SEQS,), 1, SEQ_LEN + 1), jax.random.fold_in(streams_of[3], 1), 1, SEQ_LEN).astype(jnp.int32)
    gain = jnp.clip(1.0 + 0.18 * jax.random.normal(streams_of[4], (D,), jnp.float32), 0.1, 1.9)
    return {"embeds": embeds, "dest_device": dest_device, "shuffle_key": shuffle_key, "lengths": lengths, "gain": gain}


def normalize(rows, tile_ids, lengths, gain):
    values = rows.astype(jnp.float32)
    meansq = lax.optimization_barrier(jnp.mean(values * values, axis=-1, keepdims=True))
    scaled = values * lax.rsqrt(jnp.maximum(meansq, 0.25)) * gain.astype(jnp.float32)
    limit = lengths[tile_ids // TILES_SEQ]
    position = (tile_ids % TILES_SEQ)[:, None] * TILE + jnp.arange(TILE, dtype=jnp.int32)[None, :]
    keep = position < limit[:, None]
    return jnp.where(keep[:, :, None], scaled, 0.0).astype(jnp.bfloat16)

def reference(embeds, dest_device, shuffle_key, lengths, gain):
    tile_ids = jnp.arange(TILES, dtype=jnp.int32)
    normed = normalize(embeds, tile_ids, lengths, gain)
    same = dest_device[:, None] == dest_device[None, :]
    earlier = shuffle_key[None, :] < shuffle_key[:, None]
    rank = lax.optimization_barrier(jnp.sum((same & earlier).astype(jnp.int32), axis=1)).astype(jnp.int32)
    slots = (dest_device * CAP + rank).astype(jnp.int32)
    packed = jnp.zeros((GROUPS * DEPTH * CAP, TILE, D), jnp.bfloat16)
    return packed.at[slots].set(normed)
```

```python
import functools

import jax
import jax.numpy as jnp
from jax import lax
from jax.experimental import pallas as pl
from jax.experimental.pallas import tpu as pltpu
from jax.sharding import PartitionSpec as P

MESH = pl.DeviceIdType.MESH
TILES_SEQ = 32
ROWS = 16
AHEAD = 2
PIECES = (640, 512, 512, 384)


def exchange(
    sizes,
    embeds,
    dest_hbm,
    key_hbm,
    lengths_hbm,
    gain_hbm,
    ranked,
    held,
    gain,
    fresh,
    send1,
    recv1,
    stage1,
    send2,
    recv2,
    stage2,
    note1,
    noted1,
    note2,
    noted2,
    dest,
    key,
    lengths,
    read1,
    read2,
    tile_of,
    source_of,
    place_of,
    slot_of,
    load_sem,
    send1_sem,
    recv1_sem,
    send2_sem,
    recv2_sem,
    note_sem,
    read_sem,
):
    nx, ny, nz = sizes
    groups = nx * ny
    tiles, tile_rows, width = embeds.shape
    chunks = tile_rows // ROWS
    last = chunks - 1
    gx, gy, gz = lax.axis_index("gx"), lax.axis_index("gy"), lax.axis_index("gz")
    group = gx * ny + gy
    first_tile = (group * nz + gz) * tiles

    def z_peer(step):
        half = step // 2
        away = jnp.where(lax.rem(step, 2) == 0, nz // 2 - half, nz // 2 + half)
        return lax.rem(gz + away, nz)

    away_xy = sorted(
        ((dx, dy) for dx in range(nx) for dy in range(ny) if dx or dy),
        key=lambda d: -min(d[0], nx - d[0]) - min(d[1], ny - d[1]),
    )

    def xy_peer(step):
        dx, dy = away_xy[step - 1]
        return lax.rem(gx + dx, nx), lax.rem(gy + dy, ny)

    barrier = pltpu.get_barrier_semaphore()

    @pl.loop(1, nz)
    def _(step):
        pl.semaphore_signal(
            barrier, inc=1, device_id={"gz": z_peer(step)}, device_id_type=MESH
        )

    for step in range(1, groups):
        x, y = xy_peer(step)
        pl.semaphore_signal(
            barrier, inc=1, device_id={"gx": x, "gy": y}, device_id_type=MESH
        )

    first_rows = pl.ds(0, ROWS)
    other_rows = pl.ds(ROWS, tile_rows - ROWS)
    loads = [
        pltpu.make_async_copy(src, dst, load_sem.at[i])
        for i, (src, dst) in enumerate(
            (
                (dest_hbm, dest),
                (key_hbm, key),
                (lengths_hbm, lengths),
                (gain_hbm, gain),
                (embeds.at[:, first_rows], held.at[:, first_rows]),
                (embeds.at[:, other_rows], held.at[:, other_rows]),
            )
        )
    ]
    for load in loads:
        load.start()

    stage1[nz] = jnp.zeros(stage1.shape[1:], stage1.dtype)
    lane = lax.broadcasted_iota(jnp.int32, (1, 128), 1)
    row = lax.broadcasted_iota(jnp.int32, (ROWS, 1), 0)
    for load in loads[:4]:
        load.wait()

    @pl.loop(0, nz)
    def _(slot):
        tile = jnp.int32(-1)
        home = jnp.int32(-1)
        rank_key = jnp.int32(-1)
        for t in range(tiles):
            here = lax.rem(dest[t], nz) == slot
            tile = jnp.where(here, t, tile)
            home = jnp.where(here, lax.div(dest[t], nz), home)
            rank_key = jnp.where(here, key[t], rank_key)
        tile_of[slot] = jnp.maximum(tile, 0)
        note1[slot] = jnp.where(lane == 0, home, rank_key)

    noted1[gz] = note1[gz]

    limit = lengths[first_tile // TILES_SEQ]
    first_position = lax.rem(first_tile, TILES_SEQ) * tile_rows

    def wait_bytes(ref, count, sem):
        part = ref.at[pl.ds(0, count)]
        pltpu.make_async_copy(part, part, sem).wait()

    def whole(chunk):
        return chunk, chunk, pl.ds(0, width)

    def piece(p):
        return last, last + p, pl.ds(sum(PIECES[:p]), PIECES[p])

    def z_copy(part, step):
        chunk, sem, columns = part
        peer = z_peer(step)
        return pltpu.make_async_remote_copy(
            src_ref=send1.at[chunk, peer, :, columns],
            dst_ref=recv1.at[chunk, gz, :, columns],
            send_sem=send1_sem.at[sem],
            recv_sem=recv1_sem.at[sem],
            device_id={"gz": peer},
            device_id_type=MESH,
        )

    def xy_copy(part, step):
        chunk, sem, columns = part
        x, y = xy_peer(step)
        return pltpu.make_async_remote_copy(
            src_ref=send2.at[chunk, x * ny + y, :, columns],
            dst_ref=recv2.at[chunk, group, :, columns],
            send_sem=send2_sem.at[sem],
            recv_sem=recv2_sem.at[sem],
            device_id={"gx": x, "gy": y},
            device_id_type=MESH,
        )

    def make_chunk(chunk):
        start = pl.multiple_of(chunk * ROWS, ROWS)
        for t in range(tiles):
            values = held[t, pl.ds(start, ROWS), :].astype(jnp.float32)
            meansq = jnp.mean(values * values, axis=-1, keepdims=True)
            scaled = values * lax.rsqrt(jnp.maximum(meansq, 0.25)) * gain[...]
            position = first_position + t * tile_rows + start + row
            fresh[t] = jnp.where(position < limit, scaled, 0.0).astype(jnp.bfloat16)
        for step in range(1, nz):
            peer = z_peer(step)
            send1[chunk, peer] = fresh[tile_of[peer]]
        recv1[chunk, gz] = fresh[tile_of[gz]]

    def send_part(part):
        for step in range(1, nz):
            z_copy(part, step).start()

    def regroup(part):
        chunk, sem, columns = part
        wait_bytes(recv1.at[chunk, :, :, columns], nz - 1, recv1_sem.at[sem])
        for slot in range(nz):
            stage1[slot, :, columns] = recv1[chunk, slot, :, columns]
        for step in range(1, groups):
            x, y = xy_peer(step)
            target = x * ny + y
            send2[chunk, target, :, columns] = stage1[source_of[target], :, columns]
        recv2[chunk, group, :, columns] = stage1[source_of[group], :, columns]

        for step in range(1, groups):
            xy_copy(part, step).start()

    def finish(part):
        chunk, sem, columns = part
        wait_bytes(recv2.at[chunk, :, :, columns], groups - 1, recv2_sem.at[sem])
        for slot in range(groups):
            stage2[slot, :, columns] = recv2[chunk, slot, :, columns]
        start = pl.multiple_of(chunk * ROWS, ROWS)
        for place in range(groups):
            ranked[place, pl.ds(start, ROWS), columns] = stage2[
                slot_of[place], :, columns
            ]

    loads[4].wait()
    make_chunk(0)
    pl.semaphore_wait(barrier, nz + groups - 2)
    send_part(whole(0))

    def note1_copy(step):
        peer = z_peer(step)
        return pltpu.make_async_remote_copy(
            src_ref=note1.at[peer],
            dst_ref=noted1.at[gz],
            send_sem=note_sem.at[0],
            recv_sem=note_sem.at[1],
            device_id={"gz": peer},
            device_id_type=MESH,
        )

    def note2_copy(step):
        x, y = xy_peer(step)
        return pltpu.make_async_remote_copy(
            src_ref=note2.at[x * ny + y],
            dst_ref=noted2.at[group],
            send_sem=note_sem.at[2],
            recv_sem=note_sem.at[3],
            device_id={"gx": x, "gy": y},
            device_id_type=MESH,
        )

    @pl.loop(1, nz)
    def _(step):
        note1_copy(step).start()

    loads[5].wait()

    @pl.loop(1, AHEAD)
    def _(chunk):
        make_chunk(chunk)
        send_part(whole(chunk))

    wait_bytes(noted1, nz - 1, note_sem.at[1])
    read = pltpu.make_async_copy(noted1, read1, read_sem.at[0])
    read.start()
    read.wait()

    @pl.loop(0, groups)
    def _(target):
        source = jnp.int32(nz)
        rank_key = jnp.int32(-1)
        for s in range(nz):
            here = read1[s, 0, 0] == target
            source = jnp.where(here, s, source)
            rank_key = jnp.where(here, read1[s, 0, 1], rank_key)
        source_of[target] = source
        note2[target] = jnp.full((1, 128), rank_key, jnp.int32)

    noted2[group] = note2[group]

    for step in range(1, groups):
        note2_copy(step).start()

    make_chunk(AHEAD)
    send_part(whole(AHEAD))
    regroup(whole(0))

    wait_bytes(noted2, groups - 1, note_sem.at[3])
    read = pltpu.make_async_copy(noted2, read2, read_sem.at[1])
    read.start()
    read.wait()

    @pl.loop(0, groups)
    def _(slot):
        mine = read2[slot, 0, 0]
        place = jnp.int32(0)
        for other in range(groups):
            theirs = read2[other, 0, 0]
            before = jnp.where(
                mine >= 0,
                (theirs >= 0) & (theirs < mine),
                (theirs >= 0) | (other < slot),
            )
            place = place + before.astype(jnp.int32)
        place_of[slot] = place

    @pl.loop(0, groups)
    def _(place):
        found = jnp.int32(0)
        for slot in range(groups):
            found = jnp.where(place_of[slot] == place, slot, found)
        slot_of[place] = found

    @pl.loop(1, last)
    def _(chunk):
        @pl.when(chunk + AHEAD < last)
        def _():
            make_chunk(chunk + AHEAD)
            send_part(whole(chunk + AHEAD))

        @pl.when(chunk + AHEAD == last)
        def _():
            make_chunk(last)
            for p in range(len(PIECES)):
                send_part(piece(p))

        regroup(whole(chunk))
        finish(whole(chunk - 1))

    regroup(piece(0))
    finish(whole(last - 1))
    for p in range(1, len(PIECES)):
        regroup(piece(p))
        finish(piece(p - 1))
    finish(piece(len(PIECES) - 1))

    wait_bytes(note1, nz - 1, note_sem.at[0])
    wait_bytes(note2, groups - 1, note_sem.at[2])

    @pl.loop(0, last)
    def _(chunk):
        wait_bytes(send1.at[chunk], nz - 1, send1_sem.at[chunk])
        wait_bytes(send2.at[chunk], groups - 1, send2_sem.at[chunk])

    for p in range(len(PIECES)):
        chunk, sem, columns = piece(p)
        wait_bytes(send1.at[chunk, :, :, columns], nz - 1, send1_sem.at[sem])
        wait_bytes(send2.at[chunk, :, :, columns], groups - 1, send2_sem.at[sem])


def solution(mesh):
    sizes = (mesh.shape["gx"], mesh.shape["gy"], mesh.shape["gz"])
    groups, nz = sizes[0] * sizes[1], sizes[2]

    def shards(embeds, dest_device, shuffle_key, lengths, gain):
        tiles, tile_rows, width = embeds.shape
        chunks = tile_rows // ROWS
        parts = chunks - 1 + len(PIECES)
        any_space = pl.BlockSpec(memory_space=pl.ANY)
        rows = lambda *lead: pltpu.VMEM((*lead, ROWS, width), jnp.bfloat16)
        notes = lambda space, count: space((count, 1, 128), jnp.int32)
        return pl.pallas_call(
            functools.partial(exchange, sizes),
            out_shape=pltpu.VMEM((groups, tile_rows, width), jnp.bfloat16),
            in_specs=[any_space] * 5,
            out_specs=pl.BlockSpec(memory_space=pltpu.VMEM),
            scratch_shapes=[
                pltpu.VMEM((tiles, tile_rows, width), jnp.bfloat16),
                pltpu.VMEM((1, width), jnp.float32),
                rows(tiles),
                rows(chunks, nz),
                rows(chunks, nz),
                rows(nz + 1),
                rows(chunks, groups),
                rows(chunks, groups),
                rows(groups),
                notes(pltpu.VMEM, nz),
                notes(pltpu.VMEM, nz),
                notes(pltpu.VMEM, groups),
                notes(pltpu.VMEM, groups),
                pltpu.SMEM(dest_device.shape, jnp.int32),
                pltpu.SMEM(shuffle_key.shape, jnp.int32),
                pltpu.SMEM(lengths.shape, jnp.int32),
                notes(pltpu.SMEM, nz),
                notes(pltpu.SMEM, groups),
                pltpu.SMEM((nz,), jnp.int32),
                pltpu.SMEM((groups,), jnp.int32),
                pltpu.SMEM((groups,), jnp.int32),
                pltpu.SMEM((groups,), jnp.int32),
                pltpu.SemaphoreType.DMA((6,)),
                pltpu.SemaphoreType.DMA((parts,)),
                pltpu.SemaphoreType.DMA((parts,)),
                pltpu.SemaphoreType.DMA((parts,)),
                pltpu.SemaphoreType.DMA((parts,)),
                pltpu.SemaphoreType.DMA((4,)),
                pltpu.SemaphoreType.DMA((2,)),
            ],
            compiler_params=pltpu.CompilerParams(
                collective_id=0, has_side_effects=True, vmem_limit_bytes=53 * 2**20
            ),
            name="exchange",
        )(embeds, dest_device, shuffle_key, lengths, gain.reshape(1, width))

    return jax.shard_map(
        shards,
        mesh=mesh,
        in_specs=(
            P(("gx", "gy", "gz"), None, None),
            P(("gx", "gy", "gz")),
            P(("gx", "gy", "gz")),
            P(),
            P(),
        ),
        out_specs=P(("gx", "gy", "gz"), None, None),
        check_vma=False,
    )
```

```python
import functools

import jax
import jax.numpy as jnp
from jax import lax
from jax.experimental import pallas as pl
from jax.experimental.pallas import tpu as pltpu
from jax.sharding import PartitionSpec as P

MESH = pl.DeviceIdType.MESH
TILES_SEQ = 32
ROWS = 16
AHEAD = 2
CORES = 2
PIECES = (640, 512, 512, 384)


def exchange(
    sizes,
    embeds,
    dest_hbm,
    key_hbm,
    lengths_hbm,
    gain_hbm,
    ranked,
    held,
    gain,
    fresh,
    send1,
    recv1,
    stage1,
    send2,
    recv2,
    stage2,
    note1,
    noted1,
    note2,
    noted2,
    dest,
    key,
    lengths,
    read1,
    read2,
    tile_of,
    source_of,
    place_of,
    slot_of,
    load_sem,
    send1_sem,
    recv1_sem,
    send2_sem,
    recv2_sem,
    note_sem,
    read_sem,
):
    nx, ny, nz = sizes
    groups = nx * ny
    tiles, tile_rows, width = embeds.shape
    chunks = tile_rows // ROWS
    last = chunks - 1
    gx, gy, gz = lax.axis_index("gx"), lax.axis_index("gy"), lax.axis_index("gz")
    group = gx * ny + gy
    first_tile = (group * nz + gz) * tiles

    def z_peer(step):
        half = step // 2
        away = jnp.where(lax.rem(step, 2) == 0, nz // 2 - half, nz // 2 + half)
        return lax.rem(gz + away, nz)

    away_xy = sorted(
        ((dx, dy) for dx in range(nx) for dy in range(ny) if dx or dy),
        key=lambda d: -min(d[0], nx - d[0]) - min(d[1], ny - d[1]),
    )

    def xy_peer(step):
        dx, dy = away_xy[step - 1]
        return lax.rem(gx + dx, nx), lax.rem(gy + dy, ny)

    barrier = pltpu.get_barrier_semaphore()

    @pl.loop(1, nz)
    def _(step):
        pl.semaphore_signal(
            barrier, inc=1, device_id={"gz": z_peer(step)}, device_id_type=MESH
        )

    for step in range(1, groups):
        x, y = xy_peer(step)
        pl.semaphore_signal(
            barrier, inc=1, device_id={"gx": x, "gy": y}, device_id_type=MESH
        )

    first_rows = pl.ds(0, ROWS)
    other_rows = pl.ds(ROWS, tile_rows - ROWS)
    loads = [
        pltpu.make_async_copy(src, dst, load_sem.at[i])
        for i, (src, dst) in enumerate(
            (
                (dest_hbm, dest),
                (key_hbm, key),
                (lengths_hbm, lengths),
                (gain_hbm, gain),
                (embeds.at[:, first_rows], held.at[:, first_rows]),
                (embeds.at[:, other_rows], held.at[:, other_rows]),
            )
        )
    ]
    for load in loads:
        load.start()

    stage1[nz] = jnp.zeros(stage1.shape[1:], stage1.dtype)
    lane = lax.broadcasted_iota(jnp.int32, (1, 128), 1)
    row = lax.broadcasted_iota(jnp.int32, (ROWS, 1), 0)
    for load in loads[:4]:
        load.wait()

    @pl.loop(0, nz)
    def _(slot):
        tile = jnp.int32(-1)
        home = jnp.int32(-1)
        rank_key = jnp.int32(-1)
        for t in range(tiles):
            here = lax.rem(dest[t], nz) == slot
            tile = jnp.where(here, t, tile)
            home = jnp.where(here, lax.div(dest[t], nz), home)
            rank_key = jnp.where(here, key[t], rank_key)
        tile_of[slot] = jnp.maximum(tile, 0)
        note1[slot] = jnp.where(lane == 0, home, rank_key)

    noted1[gz] = note1[gz]

    limit = lengths[first_tile // TILES_SEQ]
    first_position = lax.rem(first_tile, TILES_SEQ) * tile_rows

    def wait_bytes(ref, count, sem):
        part = ref.at[pl.ds(0, count)]
        pltpu.make_async_copy(part, part, sem).wait()

    def whole(chunk):
        return chunk, chunk, pl.ds(0, width)

    def piece(p):
        return last, last + p, pl.ds(sum(PIECES[:p]), PIECES[p])

    def last_peers():
        def order(me):
            def rank(peer):
                chip = peer // CORES
                away = abs(chip - me // CORES)
                return chip > 0, -min(away, nz // CORES - away), peer

            return sorted((p for p in range(nz) if p != me), key=rank)

        orders = [order(me) for me in range(nz)]
        peers = []
        for k in range(nz - 1):
            peer = jnp.int32(orders[0][k])
            for me in range(1, nz):
                peer = jnp.where(gz == me, orders[me][k], peer)
            peers.append(peer)
        return peers

    def z_copy(part, peer):
        chunk, sem, columns = part
        return pltpu.make_async_remote_copy(
            src_ref=send1.at[chunk, peer, :, columns],
            dst_ref=recv1.at[chunk, gz, :, columns],
            send_sem=send1_sem.at[sem],
            recv_sem=recv1_sem.at[sem],
            device_id={"gz": peer},
            device_id_type=MESH,
        )

    def xy_copy(part, step):
        chunk, sem, columns = part
        x, y = xy_peer(step)
        return pltpu.make_async_remote_copy(
            src_ref=send2.at[chunk, x * ny + y, :, columns],
            dst_ref=recv2.at[chunk, group, :, columns],
            send_sem=send2_sem.at[sem],
            recv_sem=recv2_sem.at[sem],
            device_id={"gx": x, "gy": y},
            device_id_type=MESH,
        )

    def make_chunk(chunk):
        start = pl.multiple_of(chunk * ROWS, ROWS)
        for t in range(tiles):
            values = held[t, pl.ds(start, ROWS), :].astype(jnp.float32)
            meansq = jnp.mean(values * values, axis=-1, keepdims=True)
            scaled = values * lax.rsqrt(jnp.maximum(meansq, 0.25)) * gain[...]
            position = first_position + t * tile_rows + start + row
            fresh[t] = jnp.where(position < limit, scaled, 0.0).astype(jnp.bfloat16)
        for step in range(1, nz):
            peer = z_peer(step)
            send1[chunk, peer] = fresh[tile_of[peer]]
        recv1[chunk, gz] = fresh[tile_of[gz]]

    def send_part(part):
        for step in range(1, nz):
            z_copy(part, z_peer(step)).start()

    def regroup(part):
        chunk, sem, columns = part
        wait_bytes(recv1.at[chunk, :, :, columns], nz - 1, recv1_sem.at[sem])
        for slot in range(nz):
            stage1[slot, :, columns] = recv1[chunk, slot, :, columns]
        for step in range(1, groups):
            x, y = xy_peer(step)
            target = x * ny + y
            send2[chunk, target, :, columns] = stage1[source_of[target], :, columns]
        recv2[chunk, group, :, columns] = stage1[source_of[group], :, columns]

        for step in range(1, groups):
            xy_copy(part, step).start()

    def finish(part):
        chunk, sem, columns = part
        wait_bytes(recv2.at[chunk, :, :, columns], groups - 1, recv2_sem.at[sem])
        for slot in range(groups):
            stage2[slot, :, columns] = recv2[chunk, slot, :, columns]
        start = pl.multiple_of(chunk * ROWS, ROWS)
        for place in range(groups):
            ranked[place, pl.ds(start, ROWS), columns] = stage2[
                slot_of[place], :, columns
            ]

    loads[4].wait()
    make_chunk(0)
    pl.semaphore_wait(barrier, nz + groups - 2)
    send_part(whole(0))

    def note1_copy(step):
        peer = z_peer(step)
        return pltpu.make_async_remote_copy(
            src_ref=note1.at[peer],
            dst_ref=noted1.at[gz],
            send_sem=note_sem.at[0],
            recv_sem=note_sem.at[1],
            device_id={"gz": peer},
            device_id_type=MESH,
        )

    def note2_copy(step):
        x, y = xy_peer(step)
        return pltpu.make_async_remote_copy(
            src_ref=note2.at[x * ny + y],
            dst_ref=noted2.at[group],
            send_sem=note_sem.at[2],
            recv_sem=note_sem.at[3],
            device_id={"gx": x, "gy": y},
            device_id_type=MESH,
        )

    @pl.loop(1, nz)
    def _(step):
        note1_copy(step).start()

    loads[5].wait()

    @pl.loop(1, AHEAD)
    def _(chunk):
        make_chunk(chunk)
        send_part(whole(chunk))

    wait_bytes(noted1, nz - 1, note_sem.at[1])
    read = pltpu.make_async_copy(noted1, read1, read_sem.at[0])
    read.start()
    read.wait()

    @pl.loop(0, groups)
    def _(target):
        source = jnp.int32(nz)
        rank_key = jnp.int32(-1)
        for s in range(nz):
            here = read1[s, 0, 0] == target
            source = jnp.where(here, s, source)
            rank_key = jnp.where(here, read1[s, 0, 1], rank_key)
        source_of[target] = source
        note2[target] = jnp.full((1, 128), rank_key, jnp.int32)

    noted2[group] = note2[group]

    for step in range(1, groups):
        note2_copy(step).start()

    make_chunk(AHEAD)
    send_part(whole(AHEAD))
    regroup(whole(0))

    wait_bytes(noted2, groups - 1, note_sem.at[3])
    read = pltpu.make_async_copy(noted2, read2, read_sem.at[1])
    read.start()
    read.wait()

    @pl.loop(0, groups)
    def _(slot):
        mine = read2[slot, 0, 0]
        place = jnp.int32(0)
        for other in range(groups):
            theirs = read2[other, 0, 0]
            before = jnp.where(
                mine >= 0,
                (theirs >= 0) & (theirs < mine),
                (theirs >= 0) | (other < slot),
            )
            place = place + before.astype(jnp.int32)
        place_of[slot] = place

    @pl.loop(0, groups)
    def _(place):
        found = jnp.int32(0)
        for slot in range(groups):
            found = jnp.where(place_of[slot] == place, slot, found)
        slot_of[place] = found

    @pl.loop(1, last)
    def _(chunk):
        @pl.when(chunk + AHEAD < last)
        def _():
            make_chunk(chunk + AHEAD)
            send_part(whole(chunk + AHEAD))

        @pl.when(chunk + AHEAD == last)
        def _():
            make_chunk(last)
            peers = last_peers()
            for p in range(len(PIECES)):
                for peer in peers:
                    z_copy(piece(p), peer).start()

        regroup(whole(chunk))
        finish(whole(chunk - 1))

    regroup(piece(0))
    finish(whole(last - 1))
    for p in range(1, len(PIECES)):
        regroup(piece(p))
        finish(piece(p - 1))
    finish(piece(len(PIECES) - 1))

    wait_bytes(note1, nz - 1, note_sem.at[0])
    wait_bytes(note2, groups - 1, note_sem.at[2])

    @pl.loop(0, last)
    def _(chunk):
        wait_bytes(send1.at[chunk], nz - 1, send1_sem.at[chunk])
        wait_bytes(send2.at[chunk], groups - 1, send2_sem.at[chunk])

    for p in range(len(PIECES)):
        chunk, sem, columns = piece(p)
        wait_bytes(send1.at[chunk, :, :, columns], nz - 1, send1_sem.at[sem])
        wait_bytes(send2.at[chunk, :, :, columns], groups - 1, send2_sem.at[sem])


def solution(mesh):
    sizes = (mesh.shape["gx"], mesh.shape["gy"], mesh.shape["gz"])
    groups, nz = sizes[0] * sizes[1], sizes[2]

    def shards(embeds, dest_device, shuffle_key, lengths, gain):
        tiles, tile_rows, width = embeds.shape
        chunks = tile_rows // ROWS
        parts = chunks - 1 + len(PIECES)
        any_space = pl.BlockSpec(memory_space=pl.ANY)
        rows = lambda *lead: pltpu.VMEM((*lead, ROWS, width), jnp.bfloat16)
        notes = lambda space, count: space((count, 1, 128), jnp.int32)
        return pl.pallas_call(
            functools.partial(exchange, sizes),
            out_shape=pltpu.VMEM((groups, tile_rows, width), jnp.bfloat16),
            in_specs=[any_space] * 5,
            out_specs=pl.BlockSpec(memory_space=pltpu.VMEM),
            scratch_shapes=[
                pltpu.VMEM((tiles, tile_rows, width), jnp.bfloat16),
                pltpu.VMEM((1, width), jnp.float32),
                rows(tiles),
                rows(chunks, nz),
                rows(chunks, nz),
                rows(nz + 1),
                rows(chunks, groups),
                rows(chunks, groups),
                rows(groups),
                notes(pltpu.VMEM, nz),
                notes(pltpu.VMEM, nz),
                notes(pltpu.VMEM, groups),
                notes(pltpu.VMEM, groups),
                pltpu.SMEM(dest_device.shape, jnp.int32),
                pltpu.SMEM(shuffle_key.shape, jnp.int32),
                pltpu.SMEM(lengths.shape, jnp.int32),
                notes(pltpu.SMEM, nz),
                notes(pltpu.SMEM, groups),
                pltpu.SMEM((nz,), jnp.int32),
                pltpu.SMEM((groups,), jnp.int32),
                pltpu.SMEM((groups,), jnp.int32),
                pltpu.SMEM((groups,), jnp.int32),
                pltpu.SemaphoreType.DMA((6,)),
                pltpu.SemaphoreType.DMA((parts,)),
                pltpu.SemaphoreType.DMA((parts,)),
                pltpu.SemaphoreType.DMA((parts,)),
                pltpu.SemaphoreType.DMA((parts,)),
                pltpu.SemaphoreType.DMA((4,)),
                pltpu.SemaphoreType.DMA((2,)),
            ],
            compiler_params=pltpu.CompilerParams(
                collective_id=0, has_side_effects=True, vmem_limit_bytes=53 * 2**20
            ),
            name="exchange",
        )(embeds, dest_device, shuffle_key, lengths, gain.reshape(1, width))

    return jax.shard_map(
        shards,
        mesh=mesh,
        in_specs=(
            P(("gx", "gy", "gz"), None, None),
            P(("gx", "gy", "gz")),
            P(("gx", "gy", "gz")),
            P(),
            P(),
        ),
        out_specs=P(("gx", "gy", "gz"), None, None),
        check_vma=False,
    )
```

```python
import functools

import jax
import jax.numpy as jnp
from jax import lax
from jax.experimental import pallas as pl
from jax.experimental.pallas import tpu as pltpu
from jax.sharding import PartitionSpec as P

MESH = pl.DeviceIdType.MESH
TILES_SEQ = 32
ROWS = 16
AHEAD = 2
CORES = 2
PIECES = (640, 512, 512, 256, 128)


def exchange(
    sizes,
    embeds,
    dest_hbm,
    key_hbm,
    lengths_hbm,
    gain_hbm,
    ranked,
    held,
    gain,
    fresh,
    send1,
    recv1,
    stage1,
    send2,
    recv2,
    stage2,
    note1,
    noted1,
    note2,
    noted2,
    dest,
    key,
    lengths,
    read1,
    read2,
    tile_of,
    source_of,
    place_of,
    slot_of,
    load_sem,
    send1_sem,
    recv1_sem,
    send2_sem,
    recv2_sem,
    note_sem,
    read_sem,
):
    nx, ny, nz = sizes
    groups = nx * ny
    tiles, tile_rows, width = embeds.shape
    chunks = tile_rows // ROWS
    last = chunks - 1
    gx, gy, gz = lax.axis_index("gx"), lax.axis_index("gy"), lax.axis_index("gz")
    group = gx * ny + gy
    first_tile = (group * nz + gz) * tiles

    def z_peer(step):
        half = step // 2
        away = jnp.where(lax.rem(step, 2) == 0, nz // 2 - half, nz // 2 + half)
        return lax.rem(gz + away, nz)

    away_xy = sorted(
        ((dx, dy) for dx in range(nx) for dy in range(ny) if dx or dy),
        key=lambda d: -min(d[0], nx - d[0]) - min(d[1], ny - d[1]),
    )

    def xy_peer(step):
        dx, dy = away_xy[step - 1]
        return lax.rem(gx + dx, nx), lax.rem(gy + dy, ny)

    barrier = pltpu.get_barrier_semaphore()

    @pl.loop(1, nz)
    def _(step):
        pl.semaphore_signal(
            barrier, inc=1, device_id={"gz": z_peer(step)}, device_id_type=MESH
        )

    for step in range(1, groups):
        x, y = xy_peer(step)
        pl.semaphore_signal(
            barrier, inc=1, device_id={"gx": x, "gy": y}, device_id_type=MESH
        )

    first_rows = pl.ds(0, ROWS)
    other_rows = pl.ds(ROWS, tile_rows - ROWS)
    loads = [
        pltpu.make_async_copy(src, dst, load_sem.at[i])
        for i, (src, dst) in enumerate(
            (
                (dest_hbm, dest),
                (key_hbm, key),
                (lengths_hbm, lengths),
                (gain_hbm, gain),
                (embeds.at[:, first_rows], held.at[:, first_rows]),
                (embeds.at[:, other_rows], held.at[:, other_rows]),
            )
        )
    ]
    for load in loads:
        load.start()

    stage1[nz] = jnp.zeros(stage1.shape[1:], stage1.dtype)
    lane = lax.broadcasted_iota(jnp.int32, (1, 128), 1)
    row = lax.broadcasted_iota(jnp.int32, (ROWS, 1), 0)
    for load in loads[:4]:
        load.wait()

    @pl.loop(0, nz)
    def _(slot):
        tile = jnp.int32(-1)
        home = jnp.int32(-1)
        rank_key = jnp.int32(-1)
        for t in range(tiles):
            here = lax.rem(dest[t], nz) == slot
            tile = jnp.where(here, t, tile)
            home = jnp.where(here, lax.div(dest[t], nz), home)
            rank_key = jnp.where(here, key[t], rank_key)
        tile_of[slot] = jnp.maximum(tile, 0)
        note1[slot] = jnp.where(lane == 0, home, rank_key)

    noted1[gz] = note1[gz]

    limit = lengths[first_tile // TILES_SEQ]
    first_position = lax.rem(first_tile, TILES_SEQ) * tile_rows

    def wait_bytes(ref, count, sem):
        part = ref.at[pl.ds(0, count)]
        pltpu.make_async_copy(part, part, sem).wait()

    def whole(chunk):
        return chunk, chunk, pl.ds(0, width)

    def piece(p):
        return last, last + p, pl.ds(sum(PIECES[:p]), PIECES[p])

    def last_peers():
        def order(me):
            def rank(peer):
                chip = peer // CORES
                away = abs(chip - me // CORES)
                return chip > 0, -min(away, nz // CORES - away), peer

            return sorted((p for p in range(nz) if p != me), key=rank)

        orders = [order(me) for me in range(nz)]
        peers = []
        for k in range(nz - 1):
            peer = jnp.int32(orders[0][k])
            for me in range(1, nz):
                peer = jnp.where(gz == me, orders[me][k], peer)
            peers.append(peer)
        return peers

    def z_copy(part, peer):
        chunk, sem, columns = part
        return pltpu.make_async_remote_copy(
            src_ref=send1.at[chunk, peer, :, columns],
            dst_ref=recv1.at[chunk, gz, :, columns],
            send_sem=send1_sem.at[sem],
            recv_sem=recv1_sem.at[sem],
            device_id={"gz": peer},
            device_id_type=MESH,
        )

    def xy_copy(part, step):
        chunk, sem, columns = part
        x, y = xy_peer(step)
        return pltpu.make_async_remote_copy(
            src_ref=send2.at[chunk, x * ny + y, :, columns],
            dst_ref=recv2.at[chunk, group, :, columns],
            send_sem=send2_sem.at[sem],
            recv_sem=recv2_sem.at[sem],
            device_id={"gx": x, "gy": y},
            device_id_type=MESH,
        )

    def make_chunk(chunk):
        start = pl.multiple_of(chunk * ROWS, ROWS)
        for t in range(tiles):
            values = held[t, pl.ds(start, ROWS), :].astype(jnp.float32)
            meansq = jnp.mean(values * values, axis=-1, keepdims=True)
            scaled = values * lax.rsqrt(jnp.maximum(meansq, 0.25)) * gain[...]
            position = first_position + t * tile_rows + start + row
            fresh[t] = jnp.where(position < limit, scaled, 0.0).astype(jnp.bfloat16)
        for step in range(1, nz):
            peer = z_peer(step)
            send1[chunk, peer] = fresh[tile_of[peer]]
        recv1[chunk, gz] = fresh[tile_of[gz]]

    def send_part(part):
        for step in range(1, nz):
            z_copy(part, z_peer(step)).start()

    def regroup(part):
        chunk, sem, columns = part
        wait_bytes(recv1.at[chunk, :, :, columns], nz - 1, recv1_sem.at[sem])
        for slot in range(nz):
            stage1[slot, :, columns] = recv1[chunk, slot, :, columns]
        for step in range(1, groups):
            x, y = xy_peer(step)
            target = x * ny + y
            send2[chunk, target, :, columns] = stage1[source_of[target], :, columns]
        recv2[chunk, group, :, columns] = stage1[source_of[group], :, columns]

        for step in range(1, groups):
            xy_copy(part, step).start()

    def finish(part):
        chunk, sem, columns = part
        wait_bytes(recv2.at[chunk, :, :, columns], groups - 1, recv2_sem.at[sem])
        for slot in range(groups):
            stage2[slot, :, columns] = recv2[chunk, slot, :, columns]
        start = pl.multiple_of(chunk * ROWS, ROWS)
        for place in range(groups):
            ranked[place, pl.ds(start, ROWS), columns] = stage2[
                slot_of[place], :, columns
            ]

    loads[4].wait()
    make_chunk(0)
    pl.semaphore_wait(barrier, nz + groups - 2)
    send_part(whole(0))

    def note1_copy(step):
        peer = z_peer(step)
        return pltpu.make_async_remote_copy(
            src_ref=note1.at[peer],
            dst_ref=noted1.at[gz],
            send_sem=note_sem.at[0],
            recv_sem=note_sem.at[1],
            device_id={"gz": peer},
            device_id_type=MESH,
        )

    def note2_copy(step):
        x, y = xy_peer(step)
        return pltpu.make_async_remote_copy(
            src_ref=note2.at[x * ny + y],
            dst_ref=noted2.at[group],
            send_sem=note_sem.at[2],
            recv_sem=note_sem.at[3],
            device_id={"gx": x, "gy": y},
            device_id_type=MESH,
        )

    @pl.loop(1, nz)
    def _(step):
        note1_copy(step).start()

    loads[5].wait()

    @pl.loop(1, AHEAD)
    def _(chunk):
        make_chunk(chunk)
        send_part(whole(chunk))

    wait_bytes(noted1, nz - 1, note_sem.at[1])
    read = pltpu.make_async_copy(noted1, read1, read_sem.at[0])
    read.start()
    read.wait()

    @pl.loop(0, groups)
    def _(target):
        source = jnp.int32(nz)
        rank_key = jnp.int32(-1)
        for s in range(nz):
            here = read1[s, 0, 0] == target
            source = jnp.where(here, s, source)
            rank_key = jnp.where(here, read1[s, 0, 1], rank_key)
        source_of[target] = source
        note2[target] = jnp.full((1, 128), rank_key, jnp.int32)

    noted2[group] = note2[group]

    for step in range(1, groups):
        note2_copy(step).start()

    make_chunk(AHEAD)
    send_part(whole(AHEAD))
    regroup(whole(0))

    wait_bytes(noted2, groups - 1, note_sem.at[3])
    read = pltpu.make_async_copy(noted2, read2, read_sem.at[1])
    read.start()
    read.wait()

    @pl.loop(0, groups)
    def _(slot):
        mine = read2[slot, 0, 0]
        place = jnp.int32(0)
        for other in range(groups):
            theirs = read2[other, 0, 0]
            before = jnp.where(
                mine >= 0,
                (theirs >= 0) & (theirs < mine),
                (theirs >= 0) | (other < slot),
            )
            place = place + before.astype(jnp.int32)
        place_of[slot] = place

    @pl.loop(0, groups)
    def _(place):
        found = jnp.int32(0)
        for slot in range(groups):
            found = jnp.where(place_of[slot] == place, slot, found)
        slot_of[place] = found

    @pl.loop(1, last)
    def _(chunk):
        @pl.when(chunk + AHEAD < last)
        def _():
            make_chunk(chunk + AHEAD)
            send_part(whole(chunk + AHEAD))

        @pl.when(chunk + AHEAD == last)
        def _():
            make_chunk(last)
            peers = last_peers()
            for p in range(len(PIECES)):
                for peer in peers:
                    z_copy(piece(p), peer).start()

        regroup(whole(chunk))
        finish(whole(chunk - 1))

    regroup(piece(0))
    finish(whole(last - 1))
    for p in range(1, len(PIECES)):
        regroup(piece(p))
    for p in range(len(PIECES)):
        finish(piece(p))

    wait_bytes(note1, nz - 1, note_sem.at[0])
    wait_bytes(note2, groups - 1, note_sem.at[2])

    @pl.loop(0, last)
    def _(chunk):
        wait_bytes(send1.at[chunk], nz - 1, send1_sem.at[chunk])
        wait_bytes(send2.at[chunk], groups - 1, send2_sem.at[chunk])

    for p in range(len(PIECES)):
        chunk, sem, columns = piece(p)
        wait_bytes(send1.at[chunk, :, :, columns], nz - 1, send1_sem.at[sem])
        wait_bytes(send2.at[chunk, :, :, columns], groups - 1, send2_sem.at[sem])


def solution(mesh):
    sizes = (mesh.shape["gx"], mesh.shape["gy"], mesh.shape["gz"])
    groups, nz = sizes[0] * sizes[1], sizes[2]

    def shards(embeds, dest_device, shuffle_key, lengths, gain):
        tiles, tile_rows, width = embeds.shape
        chunks = tile_rows // ROWS
        parts = chunks - 1 + len(PIECES)
        any_space = pl.BlockSpec(memory_space=pl.ANY)
        rows = lambda *lead: pltpu.VMEM((*lead, ROWS, width), jnp.bfloat16)
        notes = lambda space, count: space((count, 1, 128), jnp.int32)
        return pl.pallas_call(
            functools.partial(exchange, sizes),
            out_shape=pltpu.VMEM((groups, tile_rows, width), jnp.bfloat16),
            in_specs=[any_space] * 5,
            out_specs=pl.BlockSpec(memory_space=pltpu.VMEM),
            scratch_shapes=[
                pltpu.VMEM((tiles, tile_rows, width), jnp.bfloat16),
                pltpu.VMEM((1, width), jnp.float32),
                rows(tiles),
                rows(chunks, nz),
                rows(chunks, nz),
                rows(nz + 1),
                rows(chunks, groups),
                rows(chunks, groups),
                rows(groups),
                notes(pltpu.VMEM, nz),
                notes(pltpu.VMEM, nz),
                notes(pltpu.VMEM, groups),
                notes(pltpu.VMEM, groups),
                pltpu.SMEM(dest_device.shape, jnp.int32),
                pltpu.SMEM(shuffle_key.shape, jnp.int32),
                pltpu.SMEM(lengths.shape, jnp.int32),
                notes(pltpu.SMEM, nz),
                notes(pltpu.SMEM, groups),
                pltpu.SMEM((nz,), jnp.int32),
                pltpu.SMEM((groups,), jnp.int32),
                pltpu.SMEM((groups,), jnp.int32),
                pltpu.SMEM((groups,), jnp.int32),
                pltpu.SemaphoreType.DMA((6,)),
                pltpu.SemaphoreType.DMA((parts,)),
                pltpu.SemaphoreType.DMA((parts,)),
                pltpu.SemaphoreType.DMA((parts,)),
                pltpu.SemaphoreType.DMA((parts,)),
                pltpu.SemaphoreType.DMA((4,)),
                pltpu.SemaphoreType.DMA((2,)),
            ],
            compiler_params=pltpu.CompilerParams(
                collective_id=0, has_side_effects=True, vmem_limit_bytes=53 * 2**20
            ),
            name="exchange",
        )(embeds, dest_device, shuffle_key, lengths, gain.reshape(1, width))

    return jax.shard_map(
        shards,
        mesh=mesh,
        in_specs=(
            P(("gx", "gy", "gz"), None, None),
            P(("gx", "gy", "gz")),
            P(("gx", "gy", "gz")),
            P(),
            P(),
        ),
        out_specs=P(("gx", "gy", "gz"), None, None),
        check_vma=False,
    )
```

```python
import functools

import jax
import jax.numpy as jnp
from jax import lax
from jax.experimental import pallas as pl
from jax.experimental.pallas import tpu as pltpu
from jax.sharding import PartitionSpec as P

MESH = pl.DeviceIdType.MESH
TILES_SEQ = 32
ROWS = 16
AHEAD = 2
CORES = 2
STORES = 4
PIECES = (640, 512, 512, 384)


def exchange(
    sizes,
    embeds,
    dest_hbm,
    key_hbm,
    lengths_hbm,
    gain_hbm,
    ranked,
    held,
    gain,
    fresh,
    send1,
    recv1,
    stage1,
    send2,
    recv2,
    stage2,
    note1,
    noted1,
    note2,
    noted2,
    dest,
    key,
    lengths,
    read1,
    read2,
    tile_of,
    source_of,
    place_of,
    slot_of,
    load_sem,
    send1_sem,
    recv1_sem,
    send2_sem,
    recv2_sem,
    note_sem,
    read_sem,
):
    nx, ny, nz = sizes
    groups = nx * ny
    tiles, tile_rows, width = embeds.shape
    chunks = tile_rows // ROWS
    last = chunks - 1
    gx, gy, gz = lax.axis_index("gx"), lax.axis_index("gy"), lax.axis_index("gz")
    group = gx * ny + gy
    first_tile = (group * nz + gz) * tiles

    def z_peer(step):
        half = step // 2
        away = jnp.where(lax.rem(step, 2) == 0, nz // 2 - half, nz // 2 + half)
        return lax.rem(gz + away, nz)

    away_xy = sorted(
        ((dx, dy) for dx in range(nx) for dy in range(ny) if dx or dy),
        key=lambda d: -min(d[0], nx - d[0]) - min(d[1], ny - d[1]),
    )

    def xy_peer(step):
        dx, dy = away_xy[step - 1]
        return lax.rem(gx + dx, nx), lax.rem(gy + dy, ny)

    barrier = pltpu.get_barrier_semaphore()

    @pl.loop(1, nz)
    def _(step):
        pl.semaphore_signal(
            barrier, inc=1, device_id={"gz": z_peer(step)}, device_id_type=MESH
        )

    for step in range(1, groups):
        x, y = xy_peer(step)
        pl.semaphore_signal(
            barrier, inc=1, device_id={"gx": x, "gy": y}, device_id_type=MESH
        )

    first_rows = pl.ds(0, ROWS)
    other_rows = pl.ds(ROWS, tile_rows - ROWS)
    loads = [
        pltpu.make_async_copy(src, dst, load_sem.at[i])
        for i, (src, dst) in enumerate(
            (
                (dest_hbm, dest),
                (key_hbm, key),
                (lengths_hbm, lengths),
                (gain_hbm, gain),
                (embeds.at[:, first_rows], held.at[:, first_rows]),
                (embeds.at[:, other_rows], held.at[:, other_rows]),
            )
        )
    ]
    for load in loads:
        load.start()

    stage1[nz] = jnp.zeros(stage1.shape[1:], stage1.dtype)
    lane = lax.broadcasted_iota(jnp.int32, (1, 128), 1)
    row = lax.broadcasted_iota(jnp.int32, (ROWS, 1), 0)
    for load in loads[:4]:
        load.wait()

    @pl.loop(0, nz)
    def _(slot):
        tile = jnp.int32(-1)
        home = jnp.int32(-1)
        rank_key = jnp.int32(-1)
        for t in range(tiles):
            here = lax.rem(dest[t], nz) == slot
            tile = jnp.where(here, t, tile)
            home = jnp.where(here, lax.div(dest[t], nz), home)
            rank_key = jnp.where(here, key[t], rank_key)
        tile_of[slot] = jnp.maximum(tile, 0)
        note1[slot] = jnp.where(lane == 0, home, rank_key)

    noted1[gz] = note1[gz]

    limit = lengths[first_tile // TILES_SEQ]
    first_position = lax.rem(first_tile, TILES_SEQ) * tile_rows

    def wait_bytes(ref, count, sem):
        part = ref.at[pl.ds(0, count)]
        pltpu.make_async_copy(part, part, sem).wait()

    def whole(chunk):
        return chunk, chunk, pl.ds(0, width)

    def piece(p):
        return last, last + p, pl.ds(sum(PIECES[:p]), PIECES[p])

    def last_peers():
        def order(me):
            def rank(peer):
                chip = peer // CORES
                away = abs(chip - me // CORES)
                return chip > 0, -min(away, nz // CORES - away), peer

            return sorted((p for p in range(nz) if p != me), key=rank)

        orders = [order(me) for me in range(nz)]
        peers = []
        for k in range(nz - 1):
            peer = jnp.int32(orders[0][k])
            for me in range(1, nz):
                peer = jnp.where(gz == me, orders[me][k], peer)
            peers.append(peer)
        return peers

    def z_copy(part, peer):
        chunk, sem, columns = part
        return pltpu.make_async_remote_copy(
            src_ref=send1.at[chunk, peer, :, columns],
            dst_ref=recv1.at[chunk, gz, :, columns],
            send_sem=send1_sem.at[sem],
            recv_sem=recv1_sem.at[sem],
            device_id={"gz": peer},
            device_id_type=MESH,
        )

    def xy_copy(part, step):
        chunk, sem, columns = part
        x, y = xy_peer(step)
        return pltpu.make_async_remote_copy(
            src_ref=send2.at[chunk, x * ny + y, :, columns],
            dst_ref=recv2.at[chunk, group, :, columns],
            send_sem=send2_sem.at[sem],
            recv_sem=recv2_sem.at[sem],
            device_id={"gx": x, "gy": y},
            device_id_type=MESH,
        )

    def make_chunk(chunk):
        start = pl.multiple_of(chunk * ROWS, ROWS)
        for t in range(tiles):
            values = held[t, pl.ds(start, ROWS), :].astype(jnp.float32)
            meansq = jnp.mean(values * values, axis=-1, keepdims=True)
            scaled = values * lax.rsqrt(jnp.maximum(meansq, 0.25)) * gain[...]
            position = first_position + t * tile_rows + start + row
            fresh[t] = jnp.where(position < limit, scaled, 0.0).astype(jnp.bfloat16)
        for step in range(1, nz):
            peer = z_peer(step)
            send1[chunk, peer] = fresh[tile_of[peer]]
        recv1[chunk, gz] = fresh[tile_of[gz]]

    def send_part(part):
        for step in range(1, nz):
            z_copy(part, z_peer(step)).start()

    def regroup(part):
        chunk, sem, columns = part
        wait_bytes(recv1.at[chunk, :, :, columns], nz - 1, recv1_sem.at[sem])
        for slot in range(nz):
            stage1[slot, :, columns] = recv1[chunk, slot, :, columns]
        for step in range(1, groups):
            x, y = xy_peer(step)
            target = x * ny + y
            send2[chunk, target, :, columns] = stage1[source_of[target], :, columns]
        recv2[chunk, group, :, columns] = stage1[source_of[group], :, columns]

        for step in range(1, groups):
            xy_copy(part, step).start()

    def finish(part):
        chunk, sem, columns = part
        wait_bytes(recv2.at[chunk, :, :, columns], groups - 1, recv2_sem.at[sem])
        for slot in range(groups):
            stage2[slot, :, columns] = recv2[chunk, slot, :, columns]
        start = pl.multiple_of(chunk * ROWS, ROWS)
        for place in range(groups):
            ranked[place, pl.ds(start, ROWS), columns] = stage2[
                slot_of[place], :, columns
            ]

    loads[4].wait()
    make_chunk(0)
    pl.semaphore_wait(barrier, nz + groups - 2)
    send_part(whole(0))

    def note1_copy(step):
        peer = z_peer(step)
        return pltpu.make_async_remote_copy(
            src_ref=note1.at[peer],
            dst_ref=noted1.at[gz],
            send_sem=note_sem.at[0],
            recv_sem=note_sem.at[1],
            device_id={"gz": peer},
            device_id_type=MESH,
        )

    def note2_copy(step):
        x, y = xy_peer(step)
        return pltpu.make_async_remote_copy(
            src_ref=note2.at[x * ny + y],
            dst_ref=noted2.at[group],
            send_sem=note_sem.at[2],
            recv_sem=note_sem.at[3],
            device_id={"gx": x, "gy": y},
            device_id_type=MESH,
        )

    @pl.loop(1, nz)
    def _(step):
        note1_copy(step).start()

    loads[5].wait()

    @pl.loop(1, AHEAD)
    def _(chunk):
        make_chunk(chunk)
        send_part(whole(chunk))

    wait_bytes(noted1, nz - 1, note_sem.at[1])
    read = pltpu.make_async_copy(noted1, read1, read_sem.at[0])
    read.start()
    read.wait()

    @pl.loop(0, groups)
    def _(target):
        source = jnp.int32(nz)
        rank_key = jnp.int32(-1)
        for s in range(nz):
            here = read1[s, 0, 0] == target
            source = jnp.where(here, s, source)
            rank_key = jnp.where(here, read1[s, 0, 1], rank_key)
        source_of[target] = source
        note2[target] = jnp.full((1, 128), rank_key, jnp.int32)

    noted2[group] = note2[group]

    for step in range(1, groups):
        note2_copy(step).start()

    make_chunk(AHEAD)
    send_part(whole(AHEAD))
    regroup(whole(0))

    wait_bytes(noted2, groups - 1, note_sem.at[3])
    read = pltpu.make_async_copy(noted2, read2, read_sem.at[1])
    read.start()
    read.wait()

    @pl.loop(0, groups)
    def _(slot):
        mine = read2[slot, 0, 0]
        place = jnp.int32(0)
        for other in range(groups):
            theirs = read2[other, 0, 0]
            before = jnp.where(
                mine >= 0,
                (theirs >= 0) & (theirs < mine),
                (theirs >= 0) | (other < slot),
            )
            place = place + before.astype(jnp.int32)
        place_of[slot] = place

    @pl.loop(0, groups)
    def _(place):
        found = jnp.int32(0)
        for slot in range(groups):
            found = jnp.where(place_of[slot] == place, slot, found)
        slot_of[place] = found

    @pl.loop(1, last)
    def _(chunk):
        @pl.when(chunk + AHEAD < last)
        def _():
            make_chunk(chunk + AHEAD)
            send_part(whole(chunk + AHEAD))

        @pl.when(chunk + AHEAD == last)
        def _():
            make_chunk(last)
            peers = last_peers()
            for p in range(len(PIECES)):
                for peer in peers:
                    z_copy(piece(p), peer).start()

        regroup(whole(chunk))
        finish(whole(chunk - 1))

    regroup(piece(0))
    finish(whole(last - 1))
    for p in range(1, len(PIECES)):
        regroup(piece(p))
        finish(piece(p - 1))
    finish(piece(len(PIECES) - 1))

    wait_bytes(note1, nz - 1, note_sem.at[0])
    wait_bytes(note2, groups - 1, note_sem.at[2])

    @pl.loop(0, last)
    def _(chunk):
        wait_bytes(send1.at[chunk], nz - 1, send1_sem.at[chunk])
        wait_bytes(send2.at[chunk], groups - 1, send2_sem.at[chunk])

    for p in range(len(PIECES)):
        chunk, sem, columns = piece(p)
        wait_bytes(send1.at[chunk, :, :, columns], nz - 1, send1_sem.at[sem])
        wait_bytes(send2.at[chunk, :, :, columns], groups - 1, send2_sem.at[sem])


def store(ranked, packed, sem):
    each = packed.shape[0] // STORES
    copies = []
    for i in range(STORES):
        part = pl.ds(i * each, each)
        copies.append(
            pltpu.make_async_copy(ranked.at[part], packed.at[part], sem.at[i])
        )
    for copy in copies:
        copy.start()
    for copy in copies:
        copy.wait()


def solution(mesh):
    sizes = (mesh.shape["gx"], mesh.shape["gy"], mesh.shape["gz"])
    groups, nz = sizes[0] * sizes[1], sizes[2]

    def shards(embeds, dest_device, shuffle_key, lengths, gain):
        tiles, tile_rows, width = embeds.shape
        chunks = tile_rows // ROWS
        parts = chunks - 1 + len(PIECES)
        any_space = pl.BlockSpec(memory_space=pl.ANY)
        rows = lambda *lead: pltpu.VMEM((*lead, ROWS, width), jnp.bfloat16)
        notes = lambda space, count: space((count, 1, 128), jnp.int32)
        ranked = pl.pallas_call(
            functools.partial(exchange, sizes),
            out_shape=pltpu.VMEM((groups, tile_rows, width), jnp.bfloat16),
            in_specs=[any_space] * 5,
            out_specs=pl.BlockSpec(memory_space=pltpu.VMEM),
            scratch_shapes=[
                pltpu.VMEM((tiles, tile_rows, width), jnp.bfloat16),
                pltpu.VMEM((1, width), jnp.float32),
                rows(tiles),
                rows(chunks, nz),
                rows(chunks, nz),
                rows(nz + 1),
                rows(chunks, groups),
                rows(chunks, groups),
                rows(groups),
                notes(pltpu.VMEM, nz),
                notes(pltpu.VMEM, nz),
                notes(pltpu.VMEM, groups),
                notes(pltpu.VMEM, groups),
                pltpu.SMEM(dest_device.shape, jnp.int32),
                pltpu.SMEM(shuffle_key.shape, jnp.int32),
                pltpu.SMEM(lengths.shape, jnp.int32),
                notes(pltpu.SMEM, nz),
                notes(pltpu.SMEM, groups),
                pltpu.SMEM((nz,), jnp.int32),
                pltpu.SMEM((groups,), jnp.int32),
                pltpu.SMEM((groups,), jnp.int32),
                pltpu.SMEM((groups,), jnp.int32),
                pltpu.SemaphoreType.DMA((6,)),
                pltpu.SemaphoreType.DMA((parts,)),
                pltpu.SemaphoreType.DMA((parts,)),
                pltpu.SemaphoreType.DMA((parts,)),
                pltpu.SemaphoreType.DMA((parts,)),
                pltpu.SemaphoreType.DMA((4,)),
                pltpu.SemaphoreType.DMA((2,)),
            ],
            compiler_params=pltpu.CompilerParams(
                collective_id=0, has_side_effects=True, vmem_limit_bytes=53 * 2**20
            ),
            name="exchange",
        )(embeds, dest_device, shuffle_key, lengths, gain.reshape(1, width))
        return pl.pallas_call(
            store,
            out_shape=jax.ShapeDtypeStruct((groups, tile_rows, width), jnp.bfloat16),
            in_specs=[pl.BlockSpec(memory_space=pltpu.VMEM)],
            out_specs=any_space,
            scratch_shapes=[pltpu.SemaphoreType.DMA((STORES,))],
            compiler_params=pltpu.CompilerParams(vmem_limit_bytes=2**20),
            name="store",
        )(ranked)

    return jax.shard_map(
        shards,
        mesh=mesh,
        in_specs=(
            P(("gx", "gy", "gz"), None, None),
            P(("gx", "gy", "gz")),
            P(("gx", "gy", "gz")),
            P(),
            P(),
        ),
        out_specs=P(("gx", "gy", "gz"), None, None),
        check_vma=False,
    )
```
